256 devices in a mesh: seq: 16 (over x, z_lo), row: 2 (over core), col: 8 (over z_hi, y).
Axes of the slice: x: 4, y: 4, z: 8 (z_hi: 2, z_lo: 4; z = z_hi * 4 + z_lo), core: 2. Of those that a mesh axis runs over, the one named last changes fastest.
Arguments:
- tokens: bfloat16 [8192, 6144], P('seq', ('row', 'col')), may hold values from -20 to 20
- ln_gain: bfloat16 [6144], P(('row', 'col')), may hold values from 0.099609375 to 1.8984375
- ln_bias: bfloat16 [6144], P(('row', 'col')), may hold values from -1.5 to 1.5
- w_qkv: bfloat16 [3, 6144, 4096], P(None, 'row', 'col'), may hold values from -3 to 3
- w_out: bfloat16 [4096, 6144], P('col', 'row'), may hold values from -0.5 to 0.5
Outputs:
- attended: bfloat16 [8192, 6144], P('seq', ('row', 'col'))
The draws below stay inside these ranges and needn't reach their ends.
All inputs are finite; a program needn't handle non-finite values.
Results may differ from the reference program's by a relative error of at most 0.014.
Values may be sent and summed in bfloat16 or wider, within the bound.
No kernel may reach another device: no remote copies, remote signals or barrier semaphores. Data moves between devices by JAX's collectives and lax.ppermute only.
A program may use at most 128 MiB of HBM per device.

```python
import math
import jax
import jax.numpy as jnp
from jax import lax

D = 6144
H = 32
HD = 128
T_SIZE = 8192


def draw_tokens(key, part):
    subkeys = jax.random.split(key, 3)
    group_size = max(D // 48, 1)
    group_count = D // group_size
    scale_levels = jnp.exp(jax.random.uniform(subkeys[0], (T_SIZE, group_count), jnp.float32, jnp.log(0.2), jnp.log(3.0)))
    scale_levels = jnp.repeat(scale_levels, group_size, axis=1)
    offsets = 0.5 * jnp.clip(jax.random.normal(subkeys[1], (T_SIZE, 1), jnp.float32), -4.0, 4.0)
    noise = jnp.clip(jax.random.normal(subkeys[2], (T_SIZE, D), jnp.float32), -4.0, 4.0)
    values = offsets + scale_levels * noise
    return values.astype(jnp.bfloat16)


def draw_w_qkv(key, part):
    subkeys = jax.random.split(key, 1)
    base = jnp.clip(jax.random.normal(subkeys[0], (3, D, H * HD), jnp.float32), -4.0, 4.0)
    factors = jnp.array([1.4, 1.4, 1.0], jnp.float32)[:, None, None] / jnp.sqrt(jnp.float32(D))
    weights = base * factors
    return weights.astype(jnp.bfloat16)


def steps_of(own_key, dims, pieces, low, high):
    level, own = 1.0, jax.random.fold_in(own_key, 6)
    for axis_at, parts in pieces:
        draws = jnp.exp(jax.random.uniform(jax.random.fold_in(own, axis_at), (parts,), jnp.float32, low / len(pieces), high / len(pieces)))
        level = level * jnp.repeat(draws, dims[axis_at] // parts).reshape([-1 if axis == axis_at else 1 for axis in range(len(dims))])
    return level


def normal_values(rng, shape, deviation, bound, cuts=(), kind=jnp.bfloat16):
    level = steps_of(rng, shape, cuts, -0.22, 0.18) if cuts else 1.0
    drawn = jax.random.normal(rng, shape, jnp.float32) * deviation * level
    return jnp.minimum(jnp.maximum(drawn, -bound), bound).astype(kind)


def setup_inputs(seed: int = 0) -> dict:
    seeds = jax.random.split(jax.random.key(seed), 6)
    tokens = draw_tokens(jax.random.fold_in(seeds[5], 71), 0)
    ln_gain = jnp.clip(1.0 + 0.18 * jax.random.normal(seeds[1], (D,), jnp.float32), 0.099609375, 1.8984375).astype(jnp.bfloat16)
    ln_bias = normal_values(seeds[2], (D,), 0.3, 1.5, ((0, 16),))
    w_qkv = draw_w_qkv(jax.random.fold_in(seeds[5], 71), 0)
    w_out = normal_values(seeds[4], (H * HD, D), HD ** -0.5, 0.5, ((0, 8), (1, 2)))
    return dict(tokens=tokens, ln_gain=ln_gain, ln_bias=ln_bias, w_qkv=w_qkv, w_out=w_out)


EPS = 0.25

def reference(tokens, ln_gain, ln_bias, w_qkv, w_out):
    as_float = tokens.astype(jnp.float32)
    token_mean = lax.optimization_barrier(jnp.sum(as_float, axis=1, keepdims=True)) / D
    meansq = lax.optimization_barrier(jnp.sum(as_float * as_float, axis=1, keepdims=True)) / D
    normed = ((as_float - token_mean) * lax.rsqrt(meansq - token_mean * token_mean + EPS) * ln_gain.astype(jnp.float32) + ln_bias.astype(jnp.float32)).astype(jnp.bfloat16)
    query_all = jnp.dot(normed, w_qkv[0], preferred_element_type=jnp.float32).astype(jnp.bfloat16)
    key_all = jnp.dot(normed, w_qkv[1], preferred_element_type=jnp.float32).astype(jnp.bfloat16)
    value_all = jnp.dot(normed, w_qkv[2], preferred_element_type=jnp.float32).astype(jnp.bfloat16)
    score_scale = 1.0 / math.sqrt(HD)

    def one_head(head_index):
        first_col = (head_index * HD).astype(jnp.int32)
        query_head = lax.dynamic_slice_in_dim(query_all, first_col, HD, 1)
        key_head = lax.dynamic_slice_in_dim(key_all, first_col, HD, 1)
        value_head = lax.dynamic_slice_in_dim(value_all, first_col, HD, 1)
        scores = jnp.dot(query_head, key_head.T, preferred_element_type=jnp.float32) * score_scale
        weights = jnp.exp(scores - lax.optimization_barrier(jnp.max(scores, axis=1, keepdims=True)))
        rowsum = lax.optimization_barrier(jnp.sum(weights, axis=1, keepdims=True))
        blended = jnp.dot(weights.astype(jnp.bfloat16), value_head, preferred_element_type=jnp.float32) / rowsum
        return blended.astype(jnp.bfloat16)
    per_head = lax.map(one_head, jnp.arange(H, dtype=jnp.int32))
    context = jnp.transpose(per_head, (1, 0, 2)).reshape(query_all.shape[0], H * HD)
    attended = as_float + jnp.dot(context, w_out, preferred_element_type=jnp.float32)
    return attended.astype(jnp.bfloat16)
```

```python
import functools
import math

import jax
import jax.numpy as jnp
from jax import lax
from jax.experimental import pallas as pl
from jax.experimental.pallas import tpu as pltpu
from jax.sharding import Mesh
from jax.sharding import PartitionSpec as P

D = 6144
HD = 128
EPS = 0.25
F32 = jnp.float32
BF16 = jnp.bfloat16
SENT = jnp.float32
SCORE_LOG2 = math.log2(math.e) / math.sqrt(HD)
VMEM = pl.BlockSpec(memory_space=pltpu.VMEM)
SMEM = pl.BlockSpec(memory_space=pltpu.SMEM)


def shift(value, axis, by):
    size = lax.axis_size(axis)
    return lax.ppermute(value, axis, [(i, (i + by) % size) for i in range(size)])


def ring_gather(value, axis, first_half, second_half):
    before = shift(value, axis, 1)
    after = shift(value, axis, 3)
    far_first = shift(first_half(before), axis, 1)
    far_second = shift(second_half(after), axis, 3)
    return before, after, far_first, far_second


def gather_directly(value, axis):
    return tuple(shift(value, axis, by) for by in (1, 3, 2))


def call(kernel, args, out_shape, vmem_mib, cost=None, **kw):
    placed = [a if a.dtype == jnp.int32 else pltpu.with_memory_space_constraint(a, pltpu.VMEM) for a in args]
    return pl.pallas_call(
        kernel,
        in_specs=[SMEM if a.dtype == jnp.int32 else VMEM for a in args],
        out_specs=jax.tree.map(lambda _: VMEM, out_shape),
        out_shape=jax.tree.map(lambda o: pltpu.VMEM(o.shape, o.dtype), out_shape),
        compiler_params=pltpu.CompilerParams(vmem_limit_bytes=vmem_mib << 20),
        cost_estimate=cost,
        **kw,
    )(*placed)


def array(shape, dtype):
    return jax.ShapeDtypeStruct(shape, dtype)


def sums_kernel(tokens, gain, bias, out):
    x = tokens[...]
    ones = jnp.ones((8, x.shape[1]), BF16)
    add = lambda v: lax.dot_general(ones, v, (((1,), (1,)), ((), ())), preferred_element_type=F32)[0:1]
    square = x.astype(F32) * x.astype(F32)
    high = square.astype(BF16)
    low = (square - high.astype(F32)).astype(BF16)
    out[0:1, :] = add(x)
    out[1:2, :] = add(high) + add(low)
    width = gain.shape[1]
    out[2:4, :] = jnp.zeros((2, out.shape[1]), F32)
    out[2:3, :width] = gain[...].astype(F32)
    out[3:4, :width] = bias[...].astype(F32)


def project_kernel(has_acc, ids, facts, facts_away, other, *refs):
    blocks, refs = refs[:4], refs[4:]
    if has_acc:
        acc_in, w, keep, send, normed = refs
    else:
        w, acc, normed = refs
    half, width = normed.shape[0] // 2, normed.shape[1] // 4

    @pl.when(pl.program_id(0) == 0)
    def _():
        sums = other[...]
        for i in range(4):
            sums = sums + facts[i, 0:2] + facts_away[i, 0:2]
        mean = sums[0:1] / D
        inv = lax.rsqrt(sums[1:2] / D - mean * mean + EPS)
        columns = jnp.concatenate([mean, inv, jnp.zeros((6, mean.shape[1]), F32)]).T
        mean, inv = columns[:, 0:1], columns[:, 1:2]
        for i, block in enumerate(blocks):
            at = pl.ds(pl.multiple_of(ids[1 + i] * width, HD), width)
            gain, bias = facts[i, 2:3, :width], facts[i, 3:4, :width]
            normed[:, at] = ((block[...].astype(F32) - mean) * inv * gain + bias).astype(BF16)

    j, n = pl.program_id(0), w.shape[2]
    at = pl.ds(pl.multiple_of(j * n, n), n)
    part = jnp.dot(normed[...], w[0], preferred_element_type=F32)
    if has_acc:
        part = part + acc_in[:, at]
        row = ids[5]
        first, second = part[:half], part[half:]
        keep[:, at] = jnp.where(row == 0, first, second)
        send[:, at] = jnp.where(row == 0, second, first).astype(send.dtype)
    else:
        acc[:, at] = part


def project(ids, blocks, facts, facts_away, other, w_qkv, acc):
    rows, width = blocks[0].shape
    n = w_qkv.shape[2]
    has_acc = acc is not None
    args = [facts, facts_away, other, *blocks] + ([acc] if has_acc else [])
    args = [pltpu.with_memory_space_constraint(v, pltpu.VMEM) for v in args]
    in_specs = [VMEM] * len(args)
    if has_acc:
        out_shape = [pltpu.VMEM((rows // 2, 3 * n), t) for t in (F32, SENT)]
        out_specs = [VMEM] * 2
    else:
        out_shape = pltpu.VMEM((rows, 3 * n), F32)
        out_specs = VMEM
    in_specs.append(pl.BlockSpec((1, 4 * width, n), lambda j, ids: (j, ids[0], 0)))
    args.append(pltpu.with_memory_space_constraint(w_qkv, pltpu.HBM))
    return pl.pallas_call(
        functools.partial(project_kernel, has_acc),
        grid_spec=pltpu.PrefetchScalarGridSpec(
            num_scalar_prefetch=1,
            grid=(3,),
            in_specs=in_specs,
            out_specs=out_specs,
            scratch_shapes=[pltpu.VMEM((rows, 4 * width), BF16)],
        ),
        out_shape=out_shape,
        compiler_params=pltpu.CompilerParams(vmem_limit_bytes=24 << 20),
        cost_estimate=pl.CostEstimate(flops=24 * rows * width * n, bytes_accessed=24 * width * n, transcendentals=0),
    )(ids, *args)


def split_kernel(zl, keep, recv, *outs):
    for s in range(4):
        head = lax.rem(zl[0] + s, 4)
        for j in range(3):
            cols = pl.ds(pl.multiple_of(j * 512 + head * HD, HD), HD)
            outs[s][j] = (keep[:, cols] + recv[:, cols].astype(F32)).astype(BF16)


def split_heads(zl, keep, recv):
    return call(split_kernel, (zl, keep, recv), [array((3, keep.shape[0], HD), BF16)] * 4, 8)


def attend_kernel(n_kv, first, last, *refs):
    qs, refs = refs[:4], refs[4:]
    kvs, refs = refs[: 2 * n_kv], refs[2 * n_kv :]
    if not first:
        (m_in, l_in, a_in), refs = refs[:3], refs[3:]
    outs = refs
    keys = [r[...].reshape(-1, HD) for r in kvs[0::2]]
    values = [r[...].reshape(-1, HD) for r in kvs[1::2]]
    for i in range(4):
        q = qs[i][...]
        scores = [
            lax.dot_general(q, k, (((1,), (1,)), ((), ())), preferred_element_type=F32) for k in keys
        ]
        top = functools.reduce(jnp.maximum, [jnp.max(s, axis=1, keepdims=True) for s in scores])
        if not first:
            top = jnp.maximum(m_in[i][:, :1], top)
        base = top * SCORE_LOG2
        partial_sum = None
        weighted = None
        for s, v in zip(scores, values):
            p = jnp.exp2(s * SCORE_LOG2 - base)
            for c in range(0, p.shape[1], HD):
                piece = p[:, c : c + HD]
                partial_sum = piece if partial_sum is None else partial_sum + piece
            pv = jnp.dot(p.astype(BF16), v, preferred_element_type=F32)
            weighted = pv if weighted is None else weighted + pv
        if not first:
            shrink = jnp.exp2(m_in[i][:, :1] * SCORE_LOG2 - base)
            partial_sum = partial_sum + l_in[i] * shrink
            weighted = weighted + a_in[i] * shrink
        if last:
            total = jnp.sum(partial_sum, axis=1, keepdims=True)
            outs[i][...] = (weighted / total).astype(BF16)
        else:
            outs[0][i] = jnp.broadcast_to(top, weighted.shape)
            outs[1][i] = partial_sum
            outs[2][i] = weighted


def attend(qs, kvs, state, last):
    rows = qs[0].shape[0]
    n_keys = sum(k.size // HD for k, _ in kvs)
    args = [*qs]
    for k, v in kvs:
        args += [k, v]
    first = state is None
    if not first:
        args += list(state)
    out_shape = [array((rows, HD), BF16)] * 4 if last else [array((4, rows, HD), F32)] * 3
    cost = pl.CostEstimate(
        flops=16 * rows * n_keys * HD * 2, bytes_accessed=4 * n_keys * HD, transcendentals=4 * rows * n_keys
    )
    return call(functools.partial(attend_kernel, len(kvs), first, last), args, out_shape, 36, cost)


def join_kernel(zl, c0, c1, c2, c3, out):
    for s, c in enumerate((c0, c1, c2, c3)):
        head = lax.rem(zl[0] + s, 4)
        out[:, pl.ds(pl.multiple_of(head * HD, HD), HD)] = c[...]


def join_heads(zl, parts):
    return call(join_kernel, (zl, *parts), array((parts[0].shape[0], 4 * HD), BF16), 4)


def mix(contexts, weights, which):
    c0, c1, c3, c2 = contexts
    total = jnp.dot(c0[...], weights[0][which], preferred_element_type=F32)
    for c, w in ((c1, weights[1]), (c2, weights[2]), (c3, weights[3])):
        total = total + jnp.dot(c[...], w[which], preferred_element_type=F32)
    return total


def mix_send_kernel(*refs):
    refs[8][...] = mix(refs[:4], refs[4:8], 1).astype(BF16)


def mix_send(contexts, weights):
    rows, width = contexts[0].shape[0], weights[0].shape[2]
    cost = pl.CostEstimate(flops=2 * rows * 2048 * width, bytes_accessed=4096 * width, transcendentals=0)
    return call(mix_send_kernel, (*contexts, *weights), array((rows, width), BF16), 12, cost)


def mix_own_kernel(*refs):
    out = refs[-1]
    out[0] = mix(refs[0:4], refs[8:12], 0)
    out[1] = mix(refs[4:8], refs[8:12], 0)


def mix_own(own, other, weights):
    rows, width = own[0].shape[0], weights[0].shape[2]
    cost = pl.CostEstimate(flops=4 * rows * 2048 * width, bytes_accessed=4096 * width, transcendentals=0)
    return call(mix_own_kernel, (*own, *other, *weights), array((2, rows, width), F32), 12, cost)


def finish_kernel(row, tokens, own, first, second, out):
    half = tokens.shape[0] // 2
    for i, received in ((0, first), (1, second)):
        at = row[0] if i == 0 else 1 - row[0]
        rows = pl.ds(pl.multiple_of(at * half, half), half)
        out[rows, :] = (tokens[rows, :].astype(F32) + own[i] + received[...].astype(F32)).astype(BF16)


def finish(row, tokens, own, first, second):
    return pl.pallas_call(
        finish_kernel,
        in_specs=[SMEM] + [VMEM] * 4,
        out_specs=VMEM,
        out_shape=array(tokens.shape, BF16),
        name="finish",
    )(row, *(pltpu.with_memory_space_constraint(v, pltpu.VMEM) for v in (tokens, own, first, second)))


def layer(tokens, ln_gain, ln_bias, w_qkv, w_out):
    row, zh, y, zl = (lax.axis_index(a) for a in ("row", "zh", "y", "zl"))
    as_int = lambda *v: jnp.stack([jnp.asarray(u, jnp.int32) for u in v])
    rows, width = tokens.shape

    partner = shift(tokens, "zh", 1)
    near = gather_directly(tokens, "y")
    local = call(sums_kernel, (tokens, ln_gain[None, :], ln_bias[None, :]), array((4, rows), F32), 8)
    facts = jnp.stack([local, *gather_directly(local, "y")])
    facts_away = shift(facts, "zh", 1)
    other = shift(jnp.sum(facts[:, 0:2] + facts_away[:, 0:2], axis=0), "row", 1)
    away = gather_directly(partner, "y")
    order = (y, (y + 3) % 4, (y + 1) % 4, (y + 2) % 4)
    acc = project(as_int(zh, *order, row), (tokens, *near), facts, facts_away, other, w_qkv, None)
    keep, send = project(as_int(1 - zh, *order, row), (partner, *away), facts_away, facts, other, w_qkv, acc)
    recv = shift(send, "row", 1)

    zl_arr = as_int(zl)
    slabs = split_heads(zl_arr, keep, recv)
    slabs = [slabs[0]] + [shift(slabs[s], "zl", s) for s in (1, 2, 3)]
    queries = [s[0] for s in slabs]
    kv = jnp.stack([s[1:] for s in slabs], axis=1)

    w_out, _ = lax.optimization_barrier((w_out, keep))
    columns = lambda z, s: lax.dynamic_slice_in_dim(w_out, (z * 4 + (y + s) % 4) * width, width, 1)
    weights = [jnp.stack([columns(zh, s), columns(1 - zh, s)]) for s in range(4)]
    weights = [weights[0]] + [shift(weights[s], "y", s) for s in (1, 2, 3)]

    before, after, far_k, far_v = ring_gather(kv, "x", lambda v: v[0], lambda v: v[1])
    swap = lambda v: shift(v, "row", 1)
    kv2 = swap(kv)
    before2 = swap(before)
    after2 = swap(after)
    far_k2 = swap(far_k)
    far_v2 = swap(far_v)
    pair = lambda v: (v[0], v[1])
    state = attend(queries, [pair(kv), pair(kv2)], None, False)
    state = attend(queries, [pair(before), pair(after)], state, False)
    state = attend(queries, [pair(before2), pair(after2)], state, False)
    contexts = attend(queries, [(far_k, far_v), (far_k2, far_v2)], state, True)

    contexts = [contexts[0]] + [shift(contexts[s], "zl", 4 - s) for s in (1, 2, 3)]
    context = join_heads(zl_arr, contexts)
    own = (context, *gather_directly(context, "y"))
    other = tuple(swap(v) for v in own)
    first = shift(mix_send(own, weights), "zh", 1)
    second = shift(mix_send(other, weights), "zh", 1)
    own_sum = mix_own(own, other, weights)
    return finish(as_int(row), tokens, own_sum, first, second)


def solution(mesh):
    finer = Mesh(mesh.devices.reshape(4, 4, 2, 2, 4), ("x", "zl", "row", "zh", "y"))
    feature = ("row", "zh", "y")
    in_specs = (
        P(("x", "zl"), feature),
        P(feature),
        P(feature),
        P(None, "row", ("zh", "y")),
        P(("zh", "y"), "row"),
    )
    return jax.shard_map(layer, mesh=finer, in_specs=in_specs, out_specs=P(("x", "zl"), feature), check_vma=False)
```

```python
import functools
import math

import jax
import jax.numpy as jnp
from jax import lax
from jax.experimental import pallas as pl
from jax.experimental.pallas import tpu as pltpu
from jax.sharding import Mesh
from jax.sharding import PartitionSpec as P

D = 6144
HD = 128
EPS = 0.25
F32 = jnp.float32
BF16 = jnp.bfloat16
SCORE_LOG2 = math.log2(math.e) / math.sqrt(HD)
UNROLL = 4
VMEM = pl.BlockSpec(memory_space=pltpu.VMEM)
SMEM = pl.BlockSpec(memory_space=pltpu.SMEM)


def shift(value, axis, by):
    size = lax.axis_size(axis)
    return lax.ppermute(value, axis, [(i, (i + by) % size) for i in range(size)])


def ring_gather(value, axis, first_half, second_half):
    before = shift(value, axis, 1)
    after = shift(value, axis, 3)
    far_first = shift(first_half(before), axis, 1)
    far_second = shift(second_half(after), axis, 3)
    return before, after, far_first, far_second


def gather_directly(value, axis):
    return tuple(shift(value, axis, by) for by in (1, 3, 2))


def call(kernel, args, out_shape, vmem_mib, cost=None, **kw):
    placed = [a if a.dtype == jnp.int32 else pltpu.with_memory_space_constraint(a, pltpu.VMEM) for a in args]
    return pl.pallas_call(
        kernel,
        in_specs=[SMEM if a.dtype == jnp.int32 else VMEM for a in args],
        out_specs=jax.tree.map(lambda _: VMEM, out_shape),
        out_shape=jax.tree.map(lambda o: pltpu.VMEM(o.shape, o.dtype), out_shape),
        compiler_params=pltpu.CompilerParams(vmem_limit_bytes=vmem_mib << 20),
        cost_estimate=cost,
        **kw,
    )(*placed)


def array(shape, dtype):
    return jax.ShapeDtypeStruct(shape, dtype)


def sums_kernel(tokens, gain, bias, out):
    x = tokens[...]
    ones = jnp.ones((8, x.shape[1]), BF16)
    add = lambda v: lax.dot_general(ones, v, (((1,), (1,)), ((), ())), preferred_element_type=F32)[0:1]
    square = x.astype(F32) * x.astype(F32)
    high = square.astype(BF16)
    low = (square - high.astype(F32)).astype(BF16)
    out[0:1, :] = add(x)
    out[1:2, :] = add(high) + add(low)
    width = gain.shape[1]
    out[2:4, :] = jnp.zeros((2, out.shape[1]), F32)
    out[2:3, :width] = gain[...].astype(F32)
    out[3:4, :width] = bias[...].astype(F32)


def project_kernel(ids, facts, facts_away, other, *refs):
    away, near, (w_hbm, keep, send, blocks, normed, w, block_sems, sems) = refs[:4], refs[4:8], refs[8:]
    _, rows, width = blocks.shape
    half, n = rows // 2, w.shape[3]
    copies = {}
    for i, source in enumerate(near):
        copies[i] = pltpu.make_async_copy(source, blocks.at[i], block_sems.at[i])
        copies[i].start()
    for j in range(3):
        for part in range(2):
            first = pl.multiple_of((ids[0] if part == 0 else 1 - ids[0]) * 4 * width, HD)
            copies[j, part] = pltpu.make_async_copy(
                w_hbm.at[j, pl.ds(first, 4 * width)], w.at[j, part], sems.at[j, part]
            )
            copies[j, part].start()

    sums = other[...]
    for i in range(4):
        sums = sums + facts[i, 0:2] + facts_away[i, 0:2]
    mean = sums[0:1] / D
    inv = lax.rsqrt(sums[1:2] / D - mean * mean + EPS)
    columns = jnp.concatenate([mean, inv, jnp.zeros((6, rows), F32)]).T
    mean, inv = columns[:, 0:1], columns[:, 1:2]
    for part, known in enumerate((facts, facts_away)):
        for i in range(4):
            at = pl.ds(pl.multiple_of(ids[1 + i] * width, HD), width)
            gain, bias = known[i, 2:3, :width], known[i, 3:4, :width]
            if part == 0:
                copies[i].wait()
            x = (blocks[i] if part == 0 else away[i][...]).astype(F32)
            normed[part, :, at] = ((x - mean) * inv * gain + bias).astype(BF16)

    row = ids[5]
    for j in range(3):
        cols = slice(j * n, (j + 1) * n)
        copies[j, 0].wait()
        total = jnp.dot(normed[0], w[j, 0], preferred_element_type=F32)
        copies[j, 1].wait()
        total = total + jnp.dot(normed[1], w[j, 1], preferred_element_type=F32)
        first, second = total[:half], total[half:]
        keep[:, cols] = jnp.where(row == 0, first, second)
        send[:, cols] = jnp.where(row == 0, second, first).astype(send.dtype)


def project(ids, near, away, facts, facts_away, other, w_qkv):
    rows, width = near[0].shape
    n = w_qkv.shape[2]
    args = [pltpu.with_memory_space_constraint(v, pltpu.VMEM) for v in (facts, facts_away, other, *away)]
    args += [pltpu.with_memory_space_constraint(v, pltpu.HBM) for v in (*near, w_qkv)]
    return pl.pallas_call(
        project_kernel,
        in_specs=[SMEM] + [VMEM] * 7 + [pl.BlockSpec(memory_space=pltpu.HBM)] * 5,
        out_specs=[VMEM] * 2,
        scratch_shapes=[
            pltpu.VMEM((4, rows, width), BF16),
            pltpu.VMEM((2, rows, 4 * width), BF16),
            pltpu.VMEM((3, 2, 4 * width, n), BF16),
            pltpu.SemaphoreType.DMA((4,)),
            pltpu.SemaphoreType.DMA((3, 2)),
        ],
        out_shape=[pltpu.VMEM((rows // 2, 3 * n), t) for t in (F32, BF16)],
        compiler_params=pltpu.CompilerParams(vmem_limit_bytes=28 << 20),
        cost_estimate=pl.CostEstimate(flops=48 * rows * width * n, bytes_accessed=48 * width * n, transcendentals=0),
        name="project",
    )(ids, *args)


def split_kernel(zl, keep, recv, *outs):
    for s in range(4):
        head = lax.rem(zl[0] + s, 4)
        for j in range(3):
            cols = pl.ds(pl.multiple_of(j * 512 + head * HD, HD), HD)
            outs[s][j] = (keep[:, cols] + recv[:, cols].astype(F32)).astype(BF16)


def split_heads(zl, keep, recv):
    return call(split_kernel, (zl, keep, recv), [array((3, keep.shape[0], HD), BF16)] * 4, 8)


def attend_kernel(n_kv, first, last, *refs):
    q_ref, *refs = refs
    kvs, refs = refs[: 2 * n_kv], refs[2 * n_kv :]
    if not first:
        (m_in, l_in, a_in), refs = refs[:3], refs[3:]
    outs = refs
    keys = [r[...].reshape(-1, HD) for r in kvs[0::2]]
    values = [r[...].reshape(-1, HD) for r in kvs[1::2]]
    def tile(i, carry):
        q = q_ref[i]
        scores = [
            lax.dot_general(q, k, (((1,), (1,)), ((), ())), preferred_element_type=F32) for k in keys
        ]
        top = functools.reduce(jnp.maximum, [jnp.max(s, axis=1, keepdims=True) for s in scores])
        if not first:
            top = jnp.maximum(m_in[i][:, :1], top)
        base = top * SCORE_LOG2
        partial_sum = None
        weighted = None
        for s, v in zip(scores, values):
            p = jnp.exp2(s * SCORE_LOG2 - base)
            for c in range(0, p.shape[1], HD):
                piece = p[:, c : c + HD]
                partial_sum = piece if partial_sum is None else partial_sum + piece
            pv = jnp.dot(p.astype(BF16), v, preferred_element_type=F32)
            weighted = pv if weighted is None else weighted + pv
        if not first:
            shrink = jnp.exp2(m_in[i][:, :1] * SCORE_LOG2 - base)
            partial_sum = partial_sum + l_in[i] * shrink
            weighted = weighted + a_in[i] * shrink
        if last:
            total = jnp.sum(partial_sum, axis=1, keepdims=True)
            outs[0][i] = (weighted / total).astype(BF16)
        else:
            outs[0][i] = jnp.broadcast_to(top, weighted.shape)
            outs[1][i] = partial_sum
            outs[2][i] = weighted
        return carry

    lax.fori_loop(0, 4, tile, 0, unroll=UNROLL)


def attend(q, kvs, state, last):
    rows = q.shape[1]
    n_keys = sum(k.size // HD for k, _ in kvs)
    args = [q]
    for k, v in kvs:
        args += [k, v]
    first = state is None
    if not first:
        args += list(state)
    out_shape = [array((4, rows, HD), BF16)] if last else [array((4, rows, HD), F32)] * 3
    cost = pl.CostEstimate(
        flops=16 * rows * n_keys * HD * 2, bytes_accessed=4 * n_keys * HD, transcendentals=4 * rows * n_keys
    )
    return call(functools.partial(attend_kernel, len(kvs), first, last), args, out_shape, 36, cost)


def join_kernel(zl, c0, c1, c2, c3, out):
    for s, c in enumerate((c0, c1, c2, c3)):
        head = lax.rem(zl[0] + s, 4)
        out[:, pl.ds(pl.multiple_of(head * HD, HD), HD)] = c[...]


def join_heads(zl, parts):
    return call(join_kernel, (zl, *parts), array((parts[0].shape[0], 4 * HD), BF16), 4)


def mix(contexts, weights, which):
    c0, c1, c3, c2 = contexts
    total = jnp.dot(c0[...], weights[0][which], preferred_element_type=F32)
    for c, w in ((c1, weights[1]), (c2, weights[2]), (c3, weights[3])):
        total = total + jnp.dot(c[...], w[which], preferred_element_type=F32)
    return total


def mix_send_kernel(*refs):
    refs[8][...] = mix(refs[:4], refs[4:8], 1).astype(BF16)


def mix_send(contexts, weights):
    rows, width = contexts[0].shape[0], weights[0].shape[2]
    cost = pl.CostEstimate(flops=2 * rows * 2048 * width, bytes_accessed=4096 * width, transcendentals=0)
    return call(mix_send_kernel, (*contexts, *weights), array((rows, width), BF16), 12, cost)


def mix_own_kernel(*refs):
    out = refs[-1]
    out[0] = mix(refs[0:4], refs[8:12], 0)
    out[1] = mix(refs[4:8], refs[8:12], 0)


def mix_own(own, other, weights):
    rows, width = own[0].shape[0], weights[0].shape[2]
    cost = pl.CostEstimate(flops=4 * rows * 2048 * width, bytes_accessed=4096 * width, transcendentals=0)
    return call(mix_own_kernel, (*own, *other, *weights), array((2, rows, width), F32), 12, cost)


def finish_kernel(row, tokens, own, first, second, out):
    half = tokens.shape[0] // 2
    for i, received in ((0, first), (1, second)):
        at = row[0] if i == 0 else 1 - row[0]
        rows = pl.ds(pl.multiple_of(at * half, half), half)
        out[rows, :] = (tokens[rows, :].astype(F32) + own[i] + received[...].astype(F32)).astype(BF16)


def finish(row, tokens, own, first, second):
    return pl.pallas_call(
        finish_kernel,
        in_specs=[SMEM] + [VMEM] * 4,
        out_specs=VMEM,
        out_shape=array(tokens.shape, BF16),
        name="finish",
    )(row, *(pltpu.with_memory_space_constraint(v, pltpu.VMEM) for v in (tokens, own, first, second)))


def layer(tokens, ln_gain, ln_bias, w_qkv, w_out):
    row, zh, y, zl = (lax.axis_index(a) for a in ("row", "zh", "y", "zl"))
    as_int = lambda *v: jnp.stack([jnp.asarray(u, jnp.int32) for u in v])
    rows, width = tokens.shape

    partner = shift(tokens, "zh", 1)
    near = gather_directly(tokens, "y")
    local = call(sums_kernel, (tokens, ln_gain[None, :], ln_bias[None, :]), array((4, rows), F32), 8)
    facts = jnp.stack([local, *gather_directly(local, "y")])
    facts_away = shift(facts, "zh", 1)
    other = shift(jnp.sum(facts[:, 0:2] + facts_away[:, 0:2], axis=0), "row", 1)
    away = gather_directly(partner, "y")
    order = (y, (y + 3) % 4, (y + 1) % 4, (y + 2) % 4)
    keep, send = project(
        as_int(zh, *order, row), (tokens, *near), (partner, *away), facts, facts_away, other, w_qkv
    )
    recv = shift(send, "row", 1)

    zl_arr = as_int(zl)
    slabs = split_heads(zl_arr, keep, recv)
    slabs = [slabs[0]] + [shift(slabs[s], "zl", s) for s in (1, 2, 3)]
    queries = jnp.stack([s[0] for s in slabs])
    kv = jnp.stack([s[1:] for s in slabs], axis=1)

    w_out, _ = lax.optimization_barrier((w_out, keep))
    columns = lambda z, s: lax.dynamic_slice_in_dim(w_out, (z * 4 + (y + s) % 4) * width, width, 1)
    weights = [jnp.stack([columns(zh, s), columns(1 - zh, s)]) for s in range(4)]
    weights = [weights[0]] + [shift(weights[s], "y", s) for s in (1, 2, 3)]

    before, after, far_k, far_v = ring_gather(kv, "x", lambda v: v[0], lambda v: v[1])
    swap = lambda v: shift(v, "row", 1)
    kv2 = swap(kv)
    before2 = swap(before)
    after2 = swap(after)
    far_k2 = swap(far_k)
    far_v2 = swap(far_v)
    pair = lambda v: (v[0], v[1])
    state = attend(queries, [pair(kv), pair(kv2)], None, False)
    state = attend(queries, [pair(before), pair(after)], state, False)
    state = attend(queries, [pair(before2), pair(after2)], state, False)
    contexts = attend(queries, [(far_k, far_v), (far_k2, far_v2)], state, True)[0]

    contexts = [contexts[0]] + [shift(contexts[s], "zl", 4 - s) for s in (1, 2, 3)]
    context = join_heads(zl_arr, contexts)
    own = (context, *gather_directly(context, "y"))
    other = tuple(swap(v) for v in own)
    first = shift(mix_send(own, weights), "zh", 1)
    second = shift(mix_send(other, weights), "zh", 1)
    own_sum = mix_own(own, other, weights)
    return finish(as_int(row), tokens, own_sum, first, second)


def solution(mesh):
    finer = Mesh(mesh.devices.reshape(4, 4, 2, 2, 4), ("x", "zl", "row", "zh", "y"))
    feature = ("row", "zh", "y")
    in_specs = (
        P(("x", "zl"), feature),
        P(feature),
        P(feature),
        P(None, "row", ("zh", "y")),
        P(("zh", "y"), "row"),
    )
    return jax.shard_map(layer, mesh=finer, in_specs=in_specs, out_specs=P(("x", "zl"), feature), check_vma=False)
```

```python
import functools
import math

import jax
import jax.numpy as jnp
from jax import lax
from jax.experimental import pallas as pl
from jax.experimental.pallas import tpu as pltpu
from jax.sharding import Mesh
from jax.sharding import PartitionSpec as P

D = 6144
HD = 128
EPS = 0.25
F32 = jnp.float32
BF16 = jnp.bfloat16
SCORE_LOG2 = math.log2(math.e) / math.sqrt(HD)
SPLIT = 1
VMEM = pl.BlockSpec(memory_space=pltpu.VMEM)
SMEM = pl.BlockSpec(memory_space=pltpu.SMEM)


def shift(value, axis, by):
    size = lax.axis_size(axis)
    return lax.ppermute(value, axis, [(i, (i + by) % size) for i in range(size)])


def ring_gather(value, axis, first_half, second_half):
    before = shift(value, axis, 1)
    after = shift(value, axis, 3)
    far_first = shift(first_half(before), axis, 1)
    far_second = shift(second_half(after), axis, 3)
    return before, after, far_first, far_second


def gather_directly(value, axis):
    return tuple(shift(value, axis, by) for by in (1, 3, 2))


def call(kernel, args, out_shape, vmem_mib, cost=None, **kw):
    placed = [a if a.dtype == jnp.int32 else pltpu.with_memory_space_constraint(a, pltpu.VMEM) for a in args]
    return pl.pallas_call(
        kernel,
        in_specs=[SMEM if a.dtype == jnp.int32 else VMEM for a in args],
        out_specs=jax.tree.map(lambda _: VMEM, out_shape),
        out_shape=jax.tree.map(lambda o: pltpu.VMEM(o.shape, o.dtype), out_shape),
        compiler_params=pltpu.CompilerParams(vmem_limit_bytes=vmem_mib << 20),
        cost_estimate=cost,
        **kw,
    )(*placed)


def array(shape, dtype):
    return jax.ShapeDtypeStruct(shape, dtype)


def sums_kernel(tokens, gain, bias, out):
    x = tokens[...]
    ones = jnp.ones((8, x.shape[1]), BF16)
    add = lambda v: lax.dot_general(ones, v, (((1,), (1,)), ((), ())), preferred_element_type=F32)[0:1]
    square = x.astype(F32) * x.astype(F32)
    high = square.astype(BF16)
    low = (square - high.astype(F32)).astype(BF16)
    out[0:1, :] = add(x)
    out[1:2, :] = add(high) + add(low)
    width = gain.shape[1]
    out[2:4, :] = jnp.zeros((2, out.shape[1]), F32)
    out[2:3, :width] = gain[...].astype(F32)
    out[3:4, :width] = bias[...].astype(F32)


def project_kernel(ids, facts, facts_away, other, *refs):
    away, near, (w_hbm, keep, send, blocks, normed, w, stats, block_sems, sems) = refs[:4], refs[4:8], refs[8:]
    _, rows, width = blocks.shape
    half, n = rows // 2, w.shape[3]
    copies = {}
    for i, source in enumerate(near):
        copies[i] = pltpu.make_async_copy(source, blocks.at[i], block_sems.at[i])
        copies[i].start()
    for j in range(3):
        for part in range(2):
            first = pl.multiple_of((ids[0] if part == 0 else 1 - ids[0]) * 4 * width, HD)
            copies[j, part] = pltpu.make_async_copy(
                w_hbm.at[j, pl.ds(first, 4 * width)], w.at[j, part], sems.at[j, part]
            )
            copies[j, part].start()

    sums = other[...]
    for i in range(4):
        sums = sums + facts[i, 0:2] + facts_away[i, 0:2]
    mean = sums[0:1] / D
    inv = lax.rsqrt(sums[1:2] / D - mean * mean + EPS)
    stats[...] = jnp.concatenate([mean, inv, jnp.zeros((6, rows), F32)]).T
    for i in range(4):
        copies[i].wait()
    chunk = rows // 8

    def normalize(c, carry):
        at_rows = pl.ds(pl.multiple_of(c * chunk, chunk), chunk)
        mean, inv = stats[at_rows, 0:1], stats[at_rows, 1:2]
        for part, known in enumerate((facts, facts_away)):
            for i in range(4):
                at = pl.ds(pl.multiple_of(ids[1 + i] * width, HD), width)
                gain, bias = known[i, 2:3, :width], known[i, 3:4, :width]
                x = (blocks[i, at_rows] if part == 0 else away[i][at_rows]).astype(F32)
                normed[part, at_rows, at] = ((x - mean) * inv * gain + bias).astype(BF16)
        return carry

    lax.fori_loop(0, 8, normalize, 0)
    row = ids[5]

    def columns_of(j, carry):
        cols = pl.ds(pl.multiple_of(j * n, n), n)
        for part in range(2):
            first = pl.multiple_of((ids[0] if part == 0 else 1 - ids[0]) * 4 * width, HD)
            pltpu.make_async_copy(
                w_hbm.at[j, pl.ds(first, 4 * width)], w.at[j, part], sems.at[j, part]
            ).wait()
        total = jnp.dot(normed[0], w[j, 0], preferred_element_type=F32)
        total = total + jnp.dot(normed[1], w[j, 1], preferred_element_type=F32)
        first, second = total[:half], total[half:]
        keep[:, cols] = jnp.where(row == 0, first, second)
        send[:, cols] = jnp.where(row == 0, second, first).astype(send.dtype)
        return carry

    lax.fori_loop(0, 3, columns_of, 0)


def project(ids, near, away, facts, facts_away, other, w_qkv):
    rows, width = near[0].shape
    n = w_qkv.shape[2]
    args = [pltpu.with_memory_space_constraint(v, pltpu.VMEM) for v in (facts, facts_away, other, *away)]
    args += [pltpu.with_memory_space_constraint(v, pltpu.HBM) for v in (*near, w_qkv)]
    return pl.pallas_call(
        project_kernel,
        in_specs=[SMEM] + [VMEM] * 7 + [pl.BlockSpec(memory_space=pltpu.HBM)] * 5,
        out_specs=[VMEM] * 2,
        scratch_shapes=[
            pltpu.VMEM((4, rows, width), BF16),
            pltpu.VMEM((2, rows, 4 * width), BF16),
            pltpu.VMEM((3, 2, 4 * width, n), BF16),
            pltpu.VMEM((rows, 8), F32),
            pltpu.SemaphoreType.DMA((4,)),
            pltpu.SemaphoreType.DMA((3, 2)),
        ],
        out_shape=[pltpu.VMEM((rows // 2, 3 * n), t) for t in (F32, BF16)],
        compiler_params=pltpu.CompilerParams(vmem_limit_bytes=28 << 20),
        cost_estimate=pl.CostEstimate(flops=48 * rows * width * n, bytes_accessed=48 * width * n, transcendentals=0),
        name="project",
    )(ids, *args)


def split_kernel(zl, keep, recv, *outs):
    def step(j, carry):
        for s in range(4):
            head = lax.rem(zl[0] + s, 4)
            cols = pl.ds(pl.multiple_of(j * 512 + head * HD, HD), HD)
            outs[s][j] = (keep[:, cols] + recv[:, cols].astype(F32)).astype(BF16)
        return carry

    lax.fori_loop(0, 3, step, 0)


def split_heads(zl, keep, recv):
    return call(split_kernel, (zl, keep, recv), [array((3, keep.shape[0], HD), BF16)] * 4, 8)


def attend_kernel(n_kv, first, last, *refs):
    q_ref, *refs = refs
    kvs, refs = refs[: 2 * n_kv], refs[2 * n_kv :]
    if not first:
        (m_in, l_in, a_in), refs = refs[:3], refs[3:]
    outs = refs
    keys = [r[...].reshape(-1, HD) for r in kvs[0::2]]
    values = [r[...].reshape(-1, HD) for r in kvs[1::2]]
    size = q_ref.shape[1] // SPLIT

    def tile(step, carry):
        at = step // SPLIT, pl.ds(pl.multiple_of(step % SPLIT * size, size), size)
        q = q_ref[at]
        scores = [
            lax.dot_general(q, k, (((1,), (1,)), ((), ())), preferred_element_type=F32) for k in keys
        ]
        top = functools.reduce(jnp.maximum, [jnp.max(s, axis=1, keepdims=True) for s in scores])
        if not first:
            top = jnp.maximum(m_in[at][:, :1], top)
        base = top * SCORE_LOG2
        partial_sum = None
        weighted = None
        for s, v in zip(scores, values):
            p = jnp.exp2(s * SCORE_LOG2 - base)
            for c in range(0, p.shape[1], HD):
                piece = p[:, c : c + HD]
                partial_sum = piece if partial_sum is None else partial_sum + piece
            pv = jnp.dot(p.astype(BF16), v, preferred_element_type=F32)
            weighted = pv if weighted is None else weighted + pv
        if not first:
            shrink = jnp.exp2(m_in[at][:, :1] * SCORE_LOG2 - base)
            partial_sum = partial_sum + l_in[at] * shrink
            weighted = weighted + a_in[at] * shrink
        if last:
            total = jnp.sum(partial_sum, axis=1, keepdims=True)
            outs[0][at] = (weighted / total).astype(BF16)
        else:
            outs[0][at] = jnp.broadcast_to(top, weighted.shape)
            outs[1][at] = partial_sum
            outs[2][at] = weighted
        return carry

    lax.fori_loop(0, 4 * SPLIT, tile, 0, unroll=2 if last else 1)


def attend(q, kvs, state, last):
    rows = q.shape[1]
    n_keys = sum(k.size // HD for k, _ in kvs)
    args = [q]
    for k, v in kvs:
        args += [k, v]
    first = state is None
    if not first:
        args += list(state)
    out_shape = [array((4, rows, HD), BF16)] if last else [array((4, rows, HD), F32)] * 3
    cost = pl.CostEstimate(
        flops=16 * rows * n_keys * HD * 2, bytes_accessed=4 * n_keys * HD, transcendentals=4 * rows * n_keys
    )
    return call(functools.partial(attend_kernel, len(kvs), first, last), args, out_shape, 36, cost)


def join_kernel(zl, c0, c1, c2, c3, out):
    for s, c in enumerate((c0, c1, c2, c3)):
        head = lax.rem(zl[0] + s, 4)
        out[:, pl.ds(pl.multiple_of(head * HD, HD), HD)] = c[...]


def join_heads(zl, parts):
    return call(join_kernel, (zl, *parts), array((parts[0].shape[0], 4 * HD), BF16), 4)


def mix(own, rest, weights, which):
    total = jnp.dot(own[...], weights[0][which], preferred_element_type=F32)
    for i, w in ((0, 1), (1, 3), (2, 2)):
        total = total + jnp.dot(rest[i], weights[w][which], preferred_element_type=F32)
    return total


def mix_send_kernel(own, rest, *refs):
    refs[4][...] = mix(own, rest, refs[:4], 1).astype(BF16)


def mix_send(contexts, weights):
    rows, width = contexts[0].shape[0], weights[0].shape[2]
    cost = pl.CostEstimate(flops=2 * rows * 2048 * width, bytes_accessed=4096 * width, transcendentals=0)
    return call(mix_send_kernel, (*contexts, *weights), array((rows, width), BF16), 12, cost)


def mix_own_kernel(own, rest, other, other_rest, *refs):
    refs[4][0] = mix(own, rest, refs[:4], 0)
    refs[4][1] = mix(other, other_rest, refs[:4], 0)


def mix_own(own, other, weights):
    rows, width = own[0].shape[0], weights[0].shape[2]
    cost = pl.CostEstimate(flops=4 * rows * 2048 * width, bytes_accessed=4096 * width, transcendentals=0)
    return call(mix_own_kernel, (*own, *other, *weights), array((2, rows, width), F32), 12, cost)


def finish_kernel(row, tokens, own, first, second, out):
    half = tokens.shape[0] // 2
    for i, received in ((0, first), (1, second)):
        at = row[0] if i == 0 else 1 - row[0]
        rows = pl.ds(pl.multiple_of(at * half, half), half)
        out[rows, :] = (tokens[rows, :].astype(F32) + own[i] + received[...].astype(F32)).astype(BF16)


def finish(row, tokens, own, first, second):
    return pl.pallas_call(
        finish_kernel,
        in_specs=[SMEM] + [VMEM] * 4,
        out_specs=VMEM,
        out_shape=array(tokens.shape, BF16),
        name="finish",
    )(row, *(pltpu.with_memory_space_constraint(v, pltpu.VMEM) for v in (tokens, own, first, second)))


def layer(tokens, ln_gain, ln_bias, w_qkv, w_out):
    row, zh, y, zl = (lax.axis_index(a) for a in ("row", "zh", "y", "zl"))
    as_int = lambda *v: jnp.stack([jnp.asarray(u, jnp.int32) for u in v])
    rows, width = tokens.shape

    partner = shift(tokens, "zh", 1)
    near = gather_directly(tokens, "y")
    local = call(sums_kernel, (tokens, ln_gain[None, :], ln_bias[None, :]), array((4, rows), F32), 8)
    facts = jnp.stack([local, *gather_directly(local, "y")])
    facts_away = shift(facts, "zh", 1)
    other = shift(jnp.sum(facts[:, 0:2] + facts_away[:, 0:2], axis=0), "row", 1)
    away = gather_directly(partner, "y")
    order = (y, (y + 3) % 4, (y + 1) % 4, (y + 2) % 4)
    keep, send = project(
        as_int(zh, *order, row), (tokens, *near), (partner, *away), facts, facts_away, other, w_qkv
    )
    recv = shift(send, "row", 1)

    zl_arr = as_int(zl)
    slabs = split_heads(zl_arr, keep, recv)
    slabs = [slabs[0]] + [shift(slabs[s], "zl", s) for s in (1, 2, 3)]
    queries = jnp.stack([s[0] for s in slabs])
    kv = jnp.stack([s[1:] for s in slabs], axis=1)

    w_out, _ = lax.optimization_barrier((w_out, keep))
    columns = lambda z, s: lax.dynamic_slice_in_dim(w_out, (z * 4 + (y + s) % 4) * width, width, 1)
    weights = [jnp.stack([columns(zh, s), columns(1 - zh, s)]) for s in range(4)]
    weights = [weights[0]] + [shift(weights[s], "y", s) for s in (1, 2, 3)]

    before, after, far_k, far_v = ring_gather(kv, "x", lambda v: v[0], lambda v: v[1])
    swap = lambda v: shift(v, "row", 1)
    kv2 = swap(kv)
    before2 = swap(before)
    after2 = swap(after)
    far_k2 = swap(far_k)
    far_v2 = swap(far_v)
    pair = lambda v: (v[0], v[1])
    state = attend(queries, [pair(kv), pair(kv2)], None, False)
    state = attend(queries, [pair(before), pair(after)], state, False)
    state = attend(queries, [pair(before2), pair(after2)], state, False)
    contexts = attend(queries, [(far_k, far_v), (far_k2, far_v2)], state, True)[0]

    contexts = [contexts[0]] + [shift(contexts[s], "zl", 4 - s) for s in (1, 2, 3)]
    context = join_heads(zl_arr, contexts)
    own = (context, jnp.stack(gather_directly(context, "y")))
    other = tuple(swap(v) for v in own)
    first = shift(mix_send(own, weights), "zh", 1)
    second = shift(mix_send(other, weights), "zh", 1)
    own_sum = mix_own(own, other, weights)
    return finish(as_int(row), tokens, own_sum, first, second)


def solution(mesh):
    finer = Mesh(mesh.devices.reshape(4, 4, 2, 2, 4), ("x", "zl", "row", "zh", "y"))
    feature = ("row", "zh", "y")
    in_specs = (
        P(("x", "zl"), feature),
        P(feature),
        P(feature),
        P(None, "row", ("zh", "y")),
        P(("zh", "y"), "row"),
    )
    return jax.shard_map(layer, mesh=finer, in_specs=in_specs, out_specs=P(("x", "zl"), feature), check_vma=False)
```

```python
import functools
import math

import jax
import jax.numpy as jnp
from jax import lax
from jax.experimental import pallas as pl
from jax.experimental.pallas import tpu as pltpu
from jax.sharding import Mesh
from jax.sharding import PartitionSpec as P

D = 6144
HD = 128
EPS = 0.25
F32 = jnp.float32
BF16 = jnp.bfloat16
SCORE_LOG2 = math.log2(math.e) / math.sqrt(HD)
SPLIT = 1
VMEM = pl.BlockSpec(memory_space=pltpu.VMEM)
SMEM = pl.BlockSpec(memory_space=pltpu.SMEM)


def shift(value, axis, by):
    size = lax.axis_size(axis)
    return lax.ppermute(value, axis, [(i, (i + by) % size) for i in range(size)])


def ring_gather(value, axis, first_half, second_half):
    before = shift(value, axis, 1)
    after = shift(value, axis, 3)
    far_first = shift(first_half(before), axis, 1)
    far_second = shift(second_half(after), axis, 3)
    return before, after, far_first, far_second


def gather_directly(value, axis):
    return tuple(shift(value, axis, by) for by in (1, 3, 2))


def call(kernel, args, out_shape, vmem_mib, cost=None, **kw):
    placed = [a if a.dtype == jnp.int32 else pltpu.with_memory_space_constraint(a, pltpu.VMEM) for a in args]
    return pl.pallas_call(
        kernel,
        in_specs=[SMEM if a.dtype == jnp.int32 else VMEM for a in args],
        out_specs=jax.tree.map(lambda _: VMEM, out_shape),
        out_shape=jax.tree.map(lambda o: pltpu.VMEM(o.shape, o.dtype), out_shape),
        compiler_params=pltpu.CompilerParams(vmem_limit_bytes=vmem_mib << 20),
        cost_estimate=cost,
        **kw,
    )(*placed)


def array(shape, dtype):
    return jax.ShapeDtypeStruct(shape, dtype)


def sums_kernel(tokens, gain, bias, out):
    x = tokens[...]
    ones = jnp.ones((8, x.shape[1]), BF16)
    add = lambda v: lax.dot_general(ones, v, (((1,), (1,)), ((), ())), preferred_element_type=F32)[0:1]
    square = x.astype(F32) * x.astype(F32)
    high = square.astype(BF16)
    low = (square - high.astype(F32)).astype(BF16)
    out[0:1, :] = add(x)
    out[1:2, :] = add(high) + add(low)
    width = gain.shape[1]
    out[2:4, :] = jnp.zeros((2, out.shape[1]), F32)
    out[2:3, :width] = gain[...].astype(F32)
    out[3:4, :width] = bias[...].astype(F32)


def project_kernel(ids, facts, facts_away, other, *refs):
    away, near, (w_hbm, keep, send, blocks, normed, w, stats, block_sems, sems) = refs[:4], refs[4:8], refs[8:]
    _, rows, width = blocks.shape
    half, n = rows // 2, w.shape[3]
    copies = {}
    for i, source in enumerate(near):
        copies[i] = pltpu.make_async_copy(source, blocks.at[i], block_sems.at[i])
        copies[i].start()
    for j in range(3):
        for part in range(2):
            first = pl.multiple_of((ids[0] if part == 0 else 1 - ids[0]) * 4 * width, HD)
            copies[j, part] = pltpu.make_async_copy(
                w_hbm.at[j, pl.ds(first, 4 * width)], w.at[j, part], sems.at[j, part]
            )
            copies[j, part].start()

    sums = other[...]
    for i in range(4):
        sums = sums + facts[i, 0:2] + facts_away[i, 0:2]
    mean = sums[0:1] / D
    inv = lax.rsqrt(sums[1:2] / D - mean * mean + EPS)
    stats[...] = jnp.concatenate([mean, inv, jnp.zeros((6, rows), F32)]).T
    for i in range(4):
        copies[i].wait()
    chunk = rows // 8

    def normalize(c, carry):
        at_rows = pl.ds(pl.multiple_of(c * chunk, chunk), chunk)
        mean, inv = stats[at_rows, 0:1], stats[at_rows, 1:2]
        for part, known in enumerate((facts, facts_away)):
            for i in range(4):
                at = pl.ds(pl.multiple_of(ids[1 + i] * width, HD), width)
                gain, bias = known[i, 2:3, :width], known[i, 3:4, :width]
                x = (blocks[i, at_rows] if part == 0 else away[i][at_rows]).astype(F32)
                normed[part, at_rows, at] = ((x - mean) * inv * gain + bias).astype(BF16)
        return carry

    lax.fori_loop(0, 8, normalize, 0)
    row = ids[5]

    def columns_of(j, carry):
        cols = pl.ds(pl.multiple_of(j * n, n), n)
        for part in range(2):
            first = pl.multiple_of((ids[0] if part == 0 else 1 - ids[0]) * 4 * width, HD)
            pltpu.make_async_copy(
                w_hbm.at[j, pl.ds(first, 4 * width)], w.at[j, part], sems.at[j, part]
            ).wait()
        total = jnp.dot(normed[0], w[j, 0], preferred_element_type=F32)
        total = total + jnp.dot(normed[1], w[j, 1], preferred_element_type=F32)
        first, second = total[:half], total[half:]
        keep[:, cols] = jnp.where(row == 0, first, second)
        send[:, cols] = jnp.where(row == 0, second, first).astype(send.dtype)
        return carry

    lax.fori_loop(0, 3, columns_of, 0)


def project(ids, near, away, facts, facts_away, other, w_qkv):
    rows, width = near[0].shape
    n = w_qkv.shape[2]
    args = [pltpu.with_memory_space_constraint(v, pltpu.VMEM) for v in (facts, facts_away, other, *away)]
    args += [pltpu.with_memory_space_constraint(v, pltpu.HBM) for v in (*near, w_qkv)]
    return pl.pallas_call(
        project_kernel,
        in_specs=[SMEM] + [VMEM] * 7 + [pl.BlockSpec(memory_space=pltpu.HBM)] * 5,
        out_specs=[VMEM] * 2,
        scratch_shapes=[
            pltpu.VMEM((4, rows, width), BF16),
            pltpu.VMEM((2, rows, 4 * width), BF16),
            pltpu.VMEM((3, 2, 4 * width, n), BF16),
            pltpu.VMEM((rows, 8), F32),
            pltpu.SemaphoreType.DMA((4,)),
            pltpu.SemaphoreType.DMA((3, 2)),
        ],
        out_shape=[pltpu.VMEM((rows // 2, 3 * n), t) for t in (F32, BF16)],
        compiler_params=pltpu.CompilerParams(vmem_limit_bytes=28 << 20),
        cost_estimate=pl.CostEstimate(flops=48 * rows * width * n, bytes_accessed=48 * width * n, transcendentals=0),
        name="project",
    )(ids, *args)


def split_kernel(zl, keep, recv, *outs):
    def own(j, s):
        head = lax.rem(zl[0] + s, 4)
        cols = pl.ds(pl.multiple_of(j * 512 + head * HD, HD), HD)
        return (keep[:, cols] + recv[:, cols].astype(F32)).astype(BF16)

    for s in range(4):
        outs[s][...] = own(0, s)

    def step(j, carry):
        for s in range(4):
            outs[4 + s][j] = own(1 + j, s)
        return carry

    lax.fori_loop(0, 2, step, 0)


def split_heads(zl, keep, recv):
    rows = keep.shape[0]
    return call(split_kernel, (zl, keep, recv), [array((rows, HD), BF16)] * 4 + [array((2, rows, HD), BF16)] * 4, 8)


def attend_kernel(n_arrays, first, last, *refs):
    q_ref, *refs = refs
    arrays, refs = refs[:n_arrays], refs[n_arrays:]
    if not first:
        (m_in, l_in, a_in), refs = refs[:3], refs[3:]
    outs = refs
    blocks = []
    for r in arrays:
        if len(r.shape) == 5:
            blocks += [r[i, j] for i in range(r.shape[0]) for j in range(2)]
        else:
            blocks += [r[0], r[1]] if r.shape[0] == 2 else [r[...]]
    keys = [v.reshape(-1, HD) for v in blocks[0::2]]
    values = [v.reshape(-1, HD) for v in blocks[1::2]]
    size = q_ref.shape[1] // SPLIT

    def tile(step, carry):
        at = step // SPLIT, pl.ds(pl.multiple_of(step % SPLIT * size, size), size)
        q = q_ref[at]
        scores = [
            lax.dot_general(q, k, (((1,), (1,)), ((), ())), preferred_element_type=F32) for k in keys
        ]
        top = functools.reduce(jnp.maximum, [jnp.max(s, axis=1, keepdims=True) for s in scores])
        if not first:
            top = jnp.maximum(m_in[at][:, :1], top)
        base = top * SCORE_LOG2
        partial_sum = None
        weighted = None
        for s, v in zip(scores, values):
            p = jnp.exp2(s * SCORE_LOG2 - base)
            for c in range(0, p.shape[1], HD):
                piece = p[:, c : c + HD]
                partial_sum = piece if partial_sum is None else partial_sum + piece
            pv = jnp.dot(p.astype(BF16), v, preferred_element_type=F32)
            weighted = pv if weighted is None else weighted + pv
        if not first:
            shrink = jnp.exp2(m_in[at][:, :1] * SCORE_LOG2 - base)
            partial_sum = partial_sum + l_in[at] * shrink
            weighted = weighted + a_in[at] * shrink
        if last:
            total = jnp.sum(partial_sum, axis=1, keepdims=True)
            outs[0][at] = (weighted / total).astype(BF16)
        else:
            outs[0][at] = jnp.broadcast_to(top, weighted.shape)
            outs[1][at] = partial_sum
            outs[2][at] = weighted
        return carry

    lax.fori_loop(0, 4 * SPLIT, tile, 0, unroll=1)


def attend(q, arrays, state, last):
    rows = q.shape[1]
    n_keys = sum(v.size for v in arrays) // (2 * HD)
    args = [q, *arrays]
    first = state is None
    if not first:
        args += list(state)
    out_shape = [array((4, rows, HD), BF16)] if last else [array((4, rows, HD), F32)] * 3
    cost = pl.CostEstimate(
        flops=16 * rows * n_keys * HD * 2, bytes_accessed=4 * n_keys * HD, transcendentals=4 * rows * n_keys
    )
    return call(functools.partial(attend_kernel, len(arrays), first, last), args, out_shape, 36, cost)


def join_kernel(zl, c0, c1, c2, c3, out):
    for s, c in enumerate((c0, c1, c2, c3)):
        head = lax.rem(zl[0] + s, 4)
        out[:, pl.ds(pl.multiple_of(head * HD, HD), HD)] = c[...]


def join_heads(zl, parts):
    return call(join_kernel, (zl, *parts), array((parts[0].shape[0], 4 * HD), BF16), 4)


def mix(own, rest, weights, which):
    total = jnp.dot(own[...], weights[0][which], preferred_element_type=F32)
    for i, w in ((0, 1), (1, 3), (2, 2)):
        total = total + jnp.dot(rest[i], weights[w][which], preferred_element_type=F32)
    return total


def mix_send_kernel(own, rest, *refs):
    refs[4][...] = mix(own, rest, refs[:4], 1).astype(BF16)


def mix_send(contexts, weights):
    rows, width = contexts[0].shape[0], weights[0].shape[2]
    cost = pl.CostEstimate(flops=2 * rows * 2048 * width, bytes_accessed=4096 * width, transcendentals=0)
    return call(mix_send_kernel, (*contexts, *weights), array((rows, width), BF16), 12, cost)


def mix_own_kernel(own, rest, other, other_rest, *refs):
    refs[4][0] = mix(own, rest, refs[:4], 0)
    refs[4][1] = mix(other, other_rest, refs[:4], 0)


def mix_own(own, other, weights):
    rows, width = own[0].shape[0], weights[0].shape[2]
    cost = pl.CostEstimate(flops=4 * rows * 2048 * width, bytes_accessed=4096 * width, transcendentals=0)
    return call(mix_own_kernel, (*own, *other, *weights), array((2, rows, width), F32), 12, cost)


def finish_kernel(row, tokens, own, first, second, out):
    half = tokens.shape[0] // 2
    for i, received in ((0, first), (1, second)):
        at = row[0] if i == 0 else 1 - row[0]
        rows = pl.ds(pl.multiple_of(at * half, half), half)
        out[rows, :] = (tokens[rows, :].astype(F32) + own[i] + received[...].astype(F32)).astype(BF16)


def finish(row, tokens, own, first, second):
    return pl.pallas_call(
        finish_kernel,
        in_specs=[SMEM] + [VMEM] * 4,
        out_specs=VMEM,
        out_shape=array(tokens.shape, BF16),
        name="finish",
    )(row, *(pltpu.with_memory_space_constraint(v, pltpu.VMEM) for v in (tokens, own, first, second)))


def layer(tokens, ln_gain, ln_bias, w_qkv, w_out):
    row, zh, y, zl = (lax.axis_index(a) for a in ("row", "zh", "y", "zl"))
    as_int = lambda *v: jnp.stack([jnp.asarray(u, jnp.int32) for u in v])
    rows, width = tokens.shape

    partner = shift(tokens, "zh", 1)
    near = gather_directly(tokens, "y")
    local = call(sums_kernel, (tokens, ln_gain[None, :], ln_bias[None, :]), array((4, rows), F32), 8)
    facts = jnp.stack([local, *gather_directly(local, "y")])
    facts_away = shift(facts, "zh", 1)
    other = shift(jnp.sum(facts[:, 0:2] + facts_away[:, 0:2], axis=0), "row", 1)
    away = gather_directly(partner, "y")
    order = (y, (y + 3) % 4, (y + 1) % 4, (y + 2) % 4)
    keep, send = project(
        as_int(zh, *order, row), (tokens, *near), (partner, *away), facts, facts_away, other, w_qkv
    )
    recv = shift(send, "row", 1)

    zl_arr = as_int(zl)
    slabs = split_heads(zl_arr, keep, recv)
    queries, slabs = slabs[:4], slabs[4:]
    slabs = [slabs[0]] + [shift(slabs[s], "zl", s) for s in (1, 2, 3)]
    queries = [queries[0]] + [shift(queries[s], "zl", s) for s in (1, 2, 3)]
    kv = jnp.stack(slabs, axis=1)
    queries = jnp.stack(queries)

    w_out, _ = lax.optimization_barrier((w_out, keep))
    columns = lambda z, s: lax.dynamic_slice_in_dim(w_out, (z * 4 + (y + s) % 4) * width, width, 1)
    weights = [jnp.stack([columns(zh, s), columns(1 - zh, s)]) for s in range(4)]
    weights = [weights[0]] + [shift(weights[s], "y", s) for s in (1, 2, 3)]

    before, after, far_k, far_v = ring_gather(kv, "x", lambda v: v[0], lambda v: v[1])
    swap = lambda v: shift(v, "row", 1)
    kv2 = swap(kv)
    near2 = swap(jnp.stack([before, after]))
    far2 = swap(jnp.stack([far_k, far_v]))
    state = attend(queries, [kv, kv2], None, False)
    state = attend(queries, [before, after], state, False)
    state = attend(queries, [near2], state, False)
    contexts = attend(queries, [far_k, far_v, far2], state, True)[0]

    contexts = [contexts[0]] + [shift(contexts[s], "zl", 4 - s) for s in (1, 2, 3)]
    context = join_heads(zl_arr, contexts)
    own = (context, jnp.stack(gather_directly(context, "y")))
    other = tuple(swap(v) for v in own)
    first = shift(mix_send(own, weights), "zh", 1)
    second = shift(mix_send(other, weights), "zh", 1)
    own_sum = mix_own(own, other, weights)
    return finish(as_int(row), tokens, own_sum, first, second)


def solution(mesh):
    finer = Mesh(mesh.devices.reshape(4, 4, 2, 2, 4), ("x", "zl", "row", "zh", "y"))
    feature = ("row", "zh", "y")
    in_specs = (
        P(("x", "zl"), feature),
        P(feature),
        P(feature),
        P(None, "row", ("zh", "y")),
        P(("zh", "y"), "row"),
    )
    return jax.shard_map(layer, mesh=finer, in_specs=in_specs, out_specs=P(("x", "zl"), feature), check_vma=False)
```
